8 devices in a mesh: data: 1 (over z), expert: 8 (over y, x, core).
Axes of the slice: x: 2, y: 2, z: 1, core: 2. Of those that a mesh axis runs over, the one named last changes fastest.
Arguments:
- x: bfloat16 [16384, 2048], P(('data', 'expert'))
- idx: int32 [16384, 7], P(('data', 'expert'))
- g: float32 [16384, 7], P(('data', 'expert'))
- hot_tok: int32 [8192], P(('data', 'expert'))
- hot_g: float32 [8192], P(('data', 'expert'))
- ln1: float32 [2048], replicated
- wq: bfloat16 [2048, 32, 128], replicated
- wk: bfloat16 [2048, 32, 128], replicated
- wv: bfloat16 [2048, 32, 128], replicated
- wo: bfloat16 [32, 128, 2048], replicated
- ln2: float32 [2048], replicated
- w1: bfloat16 [128, 2048, 768], P('expert')
- w3: bfloat16 [128, 2048, 768], P('expert')
- w2: bfloat16 [128, 768, 2048], P('expert')
Outputs:
- output: bfloat16 [16384, 2048], P(('data', 'expert'))
All inputs are finite; a program needn't handle non-finite values.
Results may differ from the reference program's by a relative error of at most 0.0107032.
Values are sent between devices in bfloat16 or wider.
A program may use at most 1 GiB of HBM per device.

```python
import jax
import jax.numpy as jnp
from jax import lax

D = 2048
FF = 768
EXPERTS = 128
TOP = 8
HEADS = 32
HEAD = 128
TOKENS = 2048
NDEV = 8
HOT = 1024
HOT_ID = 1

KC = TOP - 1
C0 = (TOKENS * KC + EXPERTS - 2) // (EXPERTS - 1)
CAP = 8 * ((3 * C0 + 15) // 16)
EPS = 1e-6
ROPE_BASE = 10000.0


def _routing(key):
    k1, k2, k3, k4, k5 = jax.random.split(key, 5)
    d1, d2, d3 = jax.random.split(jax.random.fold_in(key, 7), 3)
    used = (EXPERTS - 1) - (EXPERTS - 1) // 3
    rank = jax.random.permutation(d1, TOKENS)
    c = (rank[:, None] * KC + jnp.arange(KC)[None, :]) % used
    cold = jax.random.permutation(d2, EXPERTS - 1)[c]
    idx = (cold + (cold >= HOT_ID)).astype(jnp.int32)
    start = jax.random.randint(d3, (), 0, TOKENS)
    hot_tok = ((start + jnp.arange(HOT)) % TOKENS).astype(jnp.int32)
    is_hot = jnp.zeros((TOKENS,), jnp.float32).at[hot_tok].set(1.0)
    lc = jax.random.normal(k4, (TOKENS, KC), jnp.float32)
    lh = jax.random.normal(k5, (TOKENS,), jnp.float32) + 1.0
    m = jnp.maximum(jnp.max(lc, axis=1), lh)
    ec = jnp.exp(lc - m[:, None])
    eh = jnp.exp(lh - m) * is_hot
    den = jnp.sum(ec, axis=1) + eh
    return idx, ec / den[:, None], hot_tok, (eh / den)[hot_tok]


def _normal(key, shape, fan_in):
    return (jax.random.normal(key, shape, jnp.float32) * fan_in ** -0.5).astype(jnp.bfloat16)


def _expert_weights(key, shape, fan_in):
    return lax.map(lambda k: _normal(k, shape, fan_in), jax.random.split(key, EXPERTS))


def setup_inputs(seed: int = 0, part: int = 0) -> dict:
    key = jax.random.PRNGKey(seed)
    ks = jax.random.split(key, 9)
    kx, kr = jax.random.split(jax.random.fold_in(key, part))
    x = jax.random.normal(kx, (NDEV * TOKENS, D), jnp.float32).astype(jnp.bfloat16)
    idx, g, hot_tok, hot_g = jax.vmap(_routing)(jax.random.split(kr, NDEV))
    return {
        'x': x,
        'idx': idx.reshape(NDEV * TOKENS, KC),
        'g': g.reshape(NDEV * TOKENS, KC),
        'hot_tok': hot_tok.reshape(NDEV * HOT),
        'hot_g': hot_g.reshape(NDEV * HOT),
        'ln1': jax.random.uniform(ks[0], (D,), jnp.float32, 0.5, 1.5),
        'wq': _normal(ks[1], (D, HEADS, HEAD), D),
        'wk': _normal(ks[2], (D, HEADS, HEAD), D),
        'wv': _normal(ks[3], (D, HEADS, HEAD), D),
        'wo': _normal(ks[4], (HEADS, HEAD, D), HEADS * HEAD),
        'ln2': jax.random.uniform(ks[5], (D,), jnp.float32, 0.5, 1.5),
        'w1': _expert_weights(ks[6], (D, FF), D),
        'w3': _expert_weights(ks[7], (D, FF), D),
        'w2': _expert_weights(ks[8], (FF, D), FF),
    }


def _rms(v, w):
    v = v.astype(jnp.float32)
    return (v * lax.rsqrt(jnp.mean(v * v, axis=-1, keepdims=True) + EPS) * w).astype(jnp.bfloat16)


def _rope(t):
    half = HEAD // 2
    freq = ROPE_BASE ** (-jnp.arange(half, dtype=jnp.float32) / half)
    ang = jnp.arange(TOKENS, dtype=jnp.float32)[:, None] * freq[None, :]
    cos = jnp.cos(ang)[:, None, :]
    sin = jnp.sin(ang)[:, None, :]
    t1, t2 = t[..., :half], t[..., half:]
    return jnp.concatenate([t1 * cos - t2 * sin, t2 * cos + t1 * sin], axis=-1)


def _attention(x, ln1, wq, wk, wv, wo):
    a = _rms(x, ln1).astype(jnp.float32)
    q = _rope(jnp.einsum('td,dhk->thk', a, wq.astype(jnp.float32))).astype(jnp.bfloat16)
    k = _rope(jnp.einsum('td,dhk->thk', a, wk.astype(jnp.float32))).astype(jnp.bfloat16)
    v = jnp.einsum('td,dhk->thk', a, wv.astype(jnp.float32)).astype(jnp.bfloat16)
    mask = jnp.tril(jnp.ones((TOKENS, TOKENS), bool))

    def head(qkv):
        qh, kh, vh = qkv
        s = jnp.dot(qh, kh.T, preferred_element_type=jnp.float32) * HEAD ** -0.5
        p = jax.nn.softmax(jnp.where(mask, s, -jnp.inf), axis=-1).astype(jnp.bfloat16)
        return jnp.dot(p, vh, preferred_element_type=jnp.float32).astype(jnp.bfloat16)

    o = lax.map(head, (q.transpose(1, 0, 2), k.transpose(1, 0, 2), v.transpose(1, 0, 2)))
    out = jnp.einsum('htk,hkd->td', o.astype(jnp.float32), wo.astype(jnp.float32))
    return (x.astype(jnp.float32) + out).astype(jnp.bfloat16)


def _ffn(a, w1, w3, w2):
    h1 = jnp.dot(a, w1, preferred_element_type=jnp.float32)
    h3 = jnp.dot(a, w3, preferred_element_type=jnp.float32)
    z = (jax.nn.silu(h1) * h3).astype(jnp.bfloat16)
    return jnp.dot(z, w2, preferred_element_type=jnp.float32).astype(jnp.bfloat16)


def reference(x, idx, g, hot_tok, hot_g, ln1, wq, wk, wv, wo, ln2, w1, w3, w2):
    h = lax.map(lambda s: _attention(s, ln1, wq, wk, wv, wo), x.reshape(NDEV, TOKENS, D))
    u = _rms(h.reshape(NDEV * TOKENS, D), ln2)
    e = idx.reshape(-1)
    r_all = e.shape[0]
    order = jnp.argsort(e, stable=True)
    counts = jnp.zeros((EXPERTS,), jnp.int32).at[e].add(1)
    starts = jnp.cumsum(counts) - counts
    gf = g.reshape(-1)
    rows = jnp.arange(NDEV * CAP)

    def body(y, ex):
        r = order[jnp.minimum(starts[ex] + rows, r_all - 1)]
        tok = r // KC
        out = _ffn(u[tok], w1[ex], w3[ex], w2[ex]).astype(jnp.float32)
        w = jnp.where(rows < counts[ex], gf[r], 0.0)
        return y.at[tok].add(w[:, None] * out), None

    y, _ = lax.scan(body, jnp.zeros((NDEV * TOKENS, D), jnp.float32), jnp.arange(EXPERTS))
    ht = hot_tok + jnp.repeat(jnp.arange(NDEV, dtype=jnp.int32) * TOKENS, HOT)
    ho = _ffn(u[ht], w1[HOT_ID], w3[HOT_ID], w2[HOT_ID]).astype(jnp.float32)
    y = y.at[ht].add(hot_g[:, None] * ho)
    return y.astype(jnp.bfloat16)
```

```python
import functools
import math

import jax
import jax.numpy as jnp
from jax import lax
from jax.experimental import pallas as pl
from jax.experimental.pallas import tpu as pltpu
from jax.sharding import PartitionSpec as P

EPS = 1e-6
ROPE_BASE = 10000.0
HOT_ID = 1
F32 = jnp.float32
BF16 = jnp.bfloat16
NQ = 4
BQ = 256
LANES = 128
VMEM_LIMIT = 60 * 1024 * 1024


def _rms(v, w):
    v = v.astype(F32)
    return (v * lax.rsqrt(jnp.mean(v * v, axis=-1, keepdims=True) + EPS) * w).astype(BF16)


def _rope_tables(n_tok, dh):
    half = dh // 2
    freq = ROPE_BASE ** (-jnp.arange(half, dtype=F32) / half)
    ang = jnp.arange(n_tok, dtype=F32)[:, None] * freq[None, :]
    cos, sin = jnp.cos(ang), jnp.sin(ang)
    return jnp.concatenate([cos, cos], axis=1), jnp.concatenate([-sin, sin], axis=1)


def _attn_kernel(chunk, tc, *refs):
    q_ref, k_ref, cos_ref, sin_ref = refs[:4]
    kp_refs, v_refs = refs[4:4 + chunk], refs[4 + chunk:5 + 2 * chunk]
    o_ref, kb_ref = refs[5 + 2 * chunk:]
    dh = q_ref.shape[-1]
    scale = dh ** -0.5 * math.log2(math.e)

    def rope(t, r):
        return (t * cos_ref[r, :] + pltpu.roll(t, dh // 2, 1) * sin_ref[r, :]).astype(BF16)

    for j in range(tc // BQ):
        r = slice(j * BQ, (j + 1) * BQ)
        kb_ref[0, r, :] = rope(k_ref[0, r, :], r)
    row = lax.broadcasted_iota(jnp.int32, (BQ, BQ), 0)
    col = lax.broadcasted_iota(jnp.int32, (BQ, BQ), 1)
    nt = (((1,), (1,)), ((), ()))
    v_ref = v_refs[chunk]
    for i in range(tc // BQ):
        r = slice(i * BQ, (i + 1) * BQ)
        q = rope(q_ref[0, r, :], r)
        pieces = [(lax.dot_general(q, kp[0], nt, preferred_element_type=F32), vp, slice(None))
                  for kp, vp in zip(kp_refs, v_refs)]
        if i:
            p = slice(0, i * BQ)
            pieces.append((lax.dot_general(q, kb_ref[0, p, :], nt, preferred_element_type=F32), v_ref, p))
        s = lax.dot_general(q, kb_ref[0, r, :], nt, preferred_element_type=F32)
        pieces.append((jnp.where(row >= col, s, -jnp.inf), v_ref, r))
        m = functools.reduce(jnp.maximum, [jnp.max(s, axis=1, keepdims=True) for s, _, _ in pieces])
        ms = m * scale
        l, o = 0.0, 0.0
        for s, vr, p in pieces:
            e = jnp.exp2(s * scale - ms)
            l = l + jnp.sum(e, axis=1, keepdims=True)
            o = o + jnp.dot(e.astype(BF16), vr[0, p, :], preferred_element_type=F32)
        o_ref[r, :] = (o / l).astype(BF16)


def _attn_chunk(chunk, q, k, cos, sin, kps, vs):
    heads, tc, dh = q.shape
    area = tc * (chunk * tc + tc // 2)
    head_block = pl.BlockSpec((1, tc, dh), lambda h: (h, 0, 0))
    table = pl.BlockSpec((tc, dh), lambda h: (chunk, 0))
    return pl.pallas_call(
        functools.partial(_attn_kernel, chunk, tc),
        grid=(heads,),
        in_specs=[head_block, head_block, table, table] + [head_block] * (2 * chunk + 1),
        out_specs=[pl.BlockSpec((tc, dh), lambda h: (0, h)), head_block],
        out_shape=[jax.ShapeDtypeStruct((tc, heads * dh), BF16),
                   jax.ShapeDtypeStruct((heads, tc, dh), BF16)],
        compiler_params=pltpu.CompilerParams(
            dimension_semantics=("arbitrary",), vmem_limit_bytes=VMEM_LIMIT),
        cost_estimate=pl.CostEstimate(
            flops=8 * heads * area * dh, bytes_accessed=heads * tc * dh * (14 + 4 * chunk),
            transcendentals=heads * area),
        name=f"attn{chunk}",
    )(q, k, cos, sin, *kps, *vs)


def _routes(idx, g, n_exp):
    t, kc = idx.shape
    key = (idx * t + jnp.arange(t, dtype=jnp.int32)[:, None]).reshape(-1)
    skey, sg = lax.sort((key, g.reshape(-1)), num_keys=1)
    e = idx.reshape(-1)
    counts = jnp.sum((e[:, None] == jnp.arange(n_exp, dtype=jnp.int32)[None, :]).astype(jnp.int32), axis=0)
    r = jnp.arange(n_exp)
    starts = jnp.sum(jnp.where(r[None, :] < r[:, None], counts[None, :], 0), axis=1)
    return lax.rem(skey, t), sg, starts, counts


def _gather_kernel(el, dev_ref, start_ref, cnt_ref, *refs):
    tok_ref, u_refs, x_ref, us_ref, rows_ref = refs[0], refs[1:-3], refs[-3], refs[-2], refs[-1]
    d = dev_ref[pl.program_id(0)]
    tc = u_refs[0].shape[1]
    for c, ref in enumerate(u_refs):
        us_ref[c * tc:(c + 1) * tc] = ref[0]

    def expert(e, _):
        n, s = cnt_ref[d, e], start_ref[d, e]

        def group(b, _):
            for i in range(16):
                rows_ref[b * 16 + i] = us_ref[tok_ref[0, 0, s + b * 16 + i]]
            o = pl.multiple_of(b * 16, 16)
            x_ref[e, 0, pl.ds(o, 16), :] = rows_ref[pl.ds(o, 16)].reshape(16, x_ref.shape[3])
            return 0

        lax.fori_loop(0, (n + 15) // 16, group, 0)
        return 0

    lax.fori_loop(0, el, expert, 0)


def _gather_rows(dev, start, cnt, tok, us, cap):
    el = start.shape[1]
    tc, s, lanes = us[0].shape[1:]
    t, dm = tc * len(us), s * lanes
    return pl.pallas_call(
        functools.partial(_gather_kernel, el),
        grid_spec=pltpu.PrefetchScalarGridSpec(
            num_scalar_prefetch=3,
            grid=(2,),
            in_specs=[pl.BlockSpec((1, 1, tok.shape[2]), lambda i, dev, *_: (dev[i], 0, 0),
                                   memory_space=pltpu.SMEM)]
            + [pl.BlockSpec((1, tc, s, lanes), lambda i, dev, *_: (dev[i], 0, 0, 0))] * len(us),
            out_specs=pl.BlockSpec((el, 1, cap, dm), lambda i, *_: (0, i, 0, 0)),
            scratch_shapes=[pltpu.VMEM((t, s, lanes), BF16), pltpu.VMEM((cap, s, lanes), BF16)],
        ),
        out_shape=jax.ShapeDtypeStruct((el, 2, cap, dm), BF16),
        compiler_params=pltpu.CompilerParams(
            dimension_semantics=("arbitrary",), vmem_limit_bytes=VMEM_LIMIT),
        cost_estimate=pl.CostEstimate(
            flops=16_000_000_000, bytes_accessed=2 * t * dm * 2 + el * 2 * cap * dm * 2, transcendentals=0),
        name="gather_rows",
    )(dev, start, cnt, tok, *us)


def _ffn_kernel(dev_ref, cnt_ref, x_ref, w1_ref, w3_ref, w2_ref, o_ref):
    e = pl.program_id(0)
    for i in range(x_ref.shape[1]):
        @pl.when(cnt_ref[dev_ref[i], e] > 0)
        def _():
            x = x_ref[0, i]
            h1 = jnp.dot(x, w1_ref[0], preferred_element_type=F32)
            h3 = jnp.dot(x, w3_ref[0], preferred_element_type=F32)
            z = (h1 * jax.nn.sigmoid(h1) * h3).astype(BF16)
            o_ref[0, i] = jnp.dot(z, w2_ref[0], preferred_element_type=F32).astype(BF16)


def _experts(dev, cnt, x, w1, w3, w2):
    el, nd, cap, dm = x.shape
    ff = w1.shape[2]
    rows = pl.BlockSpec((1, nd, cap, dm), lambda e, *_: (e, 0, 0, 0))
    return pl.pallas_call(
        _ffn_kernel,
        grid_spec=pltpu.PrefetchScalarGridSpec(
            num_scalar_prefetch=2,
            grid=(el,),
            in_specs=[rows,
                      pl.BlockSpec((1, dm, ff), lambda e, *_: (e, 0, 0)),
                      pl.BlockSpec((1, dm, ff), lambda e, *_: (e, 0, 0)),
                      pl.BlockSpec((1, ff, dm), lambda e, *_: (e, 0, 0))],
            out_specs=rows,
        ),
        out_shape=jax.ShapeDtypeStruct((el, nd, cap, dm), BF16),
        compiler_params=pltpu.CompilerParams(
            dimension_semantics=("arbitrary",), vmem_limit_bytes=VMEM_LIMIT),
        cost_estimate=pl.CostEstimate(
            flops=6 * el * nd * cap * dm * ff, bytes_accessed=4 * x.size + 6 * w1.size,
            transcendentals=el * nd * cap * ff),
        name="experts",
    )(dev, cnt, x, w1, w3, w2)


def _combine_kernel(per, has_init, dev_ref, start_ref, cnt_ref, tok_ref, g_ref, o_ref, *refs):
    inits, (ya_ref, yb_ref, fa_ref, fb_ref) = refs[:-4], refs[-4:]
    d = dev_ref[0]
    blk = pl.program_id(0)
    sub = ya_ref.shape[1]

    @pl.when(blk == 0)
    def _():
        if has_init:
            ya_ref[...] = inits[0][...]
            yb_ref[...] = inits[1][...]
        else:
            ya_ref[...] = jnp.zeros_like(ya_ref)
            yb_ref[...] = jnp.zeros_like(yb_ref)

    def expert(k, _):
        e = blk * per + k
        n, s = cnt_ref[d, e], start_ref[d, e]

        @pl.when(n > 0)
        def _():
            for j in range(sub):
                fa_ref[:, j, :] = o_ref[k, 0, :, j * LANES:(j + 1) * LANES].astype(F32)
                fb_ref[:, j, :] = o_ref[k, 0, :, (sub + j) * LANES:(sub + j + 1) * LANES].astype(F32)

            def rows(b, k):
                toks = [tok_ref[0, 0, s + b + i] for i in range(k)]
                gates = [g_ref[0, 0, s + b + i] for i in range(k)]
                na = [ya_ref[toks[i]] + gates[i] * fa_ref[b + i] for i in range(k)]
                nb = [yb_ref[toks[i]] + gates[i] * fb_ref[b + i] for i in range(k)]
                for i in range(k):
                    ya_ref[toks[i]] = na[i]
                    yb_ref[toks[i]] = nb[i]

            def group(b, _):
                rows(b * 8, 8)
                return 0

            def single(b, _):
                rows(b, 1)
                return 0

            full = n // 8
            lax.fori_loop(0, full, group, 0)
            lax.fori_loop(full * 8, n, single, 0)
        return 0

    lax.fori_loop(0, per, expert, 0)


def _combine(dev, which, start, cnt, tok, gate, o, t, init):
    el, _, cap, dm = o.shape
    sub = dm // (2 * LANES)
    per = max(el // 8, 1)
    smem = pl.BlockSpec((1, 1, tok.shape[2]), lambda b, dev, *_: (dev[0], 0, 0), memory_space=pltpu.SMEM)
    y = pl.BlockSpec((t, sub, LANES), lambda b, *_: (0, 0, 0), pipeline_mode=pl.Buffered(1))
    return pl.pallas_call(
        functools.partial(_combine_kernel, per, bool(init)),
        grid_spec=pltpu.PrefetchScalarGridSpec(
            num_scalar_prefetch=3,
            grid=(el // per,),
            in_specs=[smem, smem, pl.BlockSpec((per, 1, cap, dm), lambda b, *_: (b, which, 0, 0))]
            + [y] * len(init),
            out_specs=[pl.BlockSpec((t, sub, LANES), lambda b, *_: (0, 0, 0))] * 2,
            scratch_shapes=[pltpu.VMEM((cap, sub, LANES), F32)] * 2,
        ),
        out_shape=[jax.ShapeDtypeStruct((t, sub, LANES), F32)] * 2,
        compiler_params=pltpu.CompilerParams(
            dimension_semantics=("arbitrary",), vmem_limit_bytes=VMEM_LIMIT),
        cost_estimate=pl.CostEstimate(
            flops=16_000_000_000, bytes_accessed=o.size + t * dm * 8, transcendentals=0),
        name="combine",
    )(dev, start, cnt, tok, gate, o, *init)


def _final_kernel(*refs):
    hy_ref, parts, y_ref = refs[0], refs[1:-1], refs[-1]
    k = len(parts) // 2
    half = y_ref.shape[1] // 2
    for j in range(2):
        c = slice(j * half, (j + 1) * half)
        tot = sum(p[...] for p in parts[j * k + 1:(j + 1) * k]) + parts[j * k][...]
        y_ref[:, c] = (tot.reshape(y_ref.shape[0], half) + hy_ref[:, c]).astype(BF16)


def _final(hy, a_parts, b_parts):
    t, dm = hy.shape
    bt = 128
    sub = dm // (2 * LANES)
    part = pl.BlockSpec((bt, sub, LANES), lambda i: (i, 0, 0))
    return pl.pallas_call(
        _final_kernel,
        grid=(t // bt,),
        in_specs=[pl.BlockSpec((bt, dm), lambda i: (i, 0))] + [part] * (len(a_parts) + len(b_parts)),
        out_specs=pl.BlockSpec((bt, dm), lambda i: (i, 0)),
        out_shape=jax.ShapeDtypeStruct((t, dm), BF16),
        compiler_params=pltpu.CompilerParams(
            dimension_semantics=("arbitrary",), vmem_limit_bytes=VMEM_LIMIT),
        cost_estimate=pl.CostEstimate(flops=8 * t * dm, bytes_accessed=18 * t * dm, transcendentals=0),
        name="final_sum",
    )(hy, *a_parts, *b_parts)


def _capacity(t, kc, n_exp):
    c0 = (t * kc + n_exp - 2) // (n_exp - 1)
    return 8 * ((3 * c0 + 15) // 16)


def _ffn(a, w1, w3, w2):
    h1 = jnp.dot(a, w1, preferred_element_type=F32)
    h3 = jnp.dot(a, w3, preferred_element_type=F32)
    z = (jax.nn.silu(h1) * h3).astype(BF16)
    return jnp.dot(z, w2, preferred_element_type=F32).astype(BF16)


CORE, X, Y = 1, 2, 4


def solution(mesh):
    n = mesh.shape['expert']

    def swap(v, bit):
        return lax.ppermute(v, 'expert', [(i, i ^ bit) for i in range(n)])

    def local(x, idx, g, hot_tok, hot_g, ln1, wq, wk, wv, wo, ln2, w1, w3, w2):
        T, D = x.shape
        KC = idx.shape[1]
        H, DH = wq.shape[1:]
        el, _, FF = w1.shape
        E = el * n
        cap = -(-_capacity(T, KC, E) // 16) * 16
        owner, lh = HOT_ID // el, HOT_ID % el
        me = lax.axis_index('expert')
        tc = T // NQ
        tie = lax.optimization_barrier

        hw = jnp.stack([w1[lh], w3[lh], w2[lh].reshape(D, FF)])
        halves = [hw[:, :D // 2], hw[:, D // 2:]]

        def spread(ws, bits, have):
            out = []
            for w, b, hv in zip(ws, bits, have):
                got = lax.ppermute(w, 'expert', [(i, i ^ b) for i in hv])
                new = functools.reduce(jnp.logical_or, [me == (i ^ b) for i in hv])
                out.append(jnp.where(new, got, w))
            return out, [hv + [i ^ b for i in hv] for b, hv in zip(bits, have)]

        have = [[owner], [owner]]

        cos, sin = _rope_tables(T, DH)
        wom = wo.reshape(H * DH, D)
        us, ug, kps, vs = [], [], [], []
        xs = [x[c * tc:(c + 1) * tc] for c in range(NQ)]
        pad = -(-(T * KC + 32) // LANES) * LANES - T * KC
        for c in range(NQ):
            a = _rms(xs[c], ln1)
            q = jnp.einsum('td,dhk->htk', a, wq, preferred_element_type=F32)
            k = jnp.einsum('td,dhk->htk', a, wk, preferred_element_type=F32)
            v = jnp.einsum('td,dhk->htk', a, wv, preferred_element_type=F32).astype(BF16)
            vs.append(v)
            o, kb = _attn_chunk(c, q, k, cos, sin, kps, vs)
            kps.append(kb)
            if c == 0:
                halves, have = spread(halves, (X, Y), have)
                o, *halves = tie((o, *halves))
            elif c == 1:
                halves, have = spread(halves, (Y, X), have)
                o, *halves = tie((o, *halves))
            elif c == 2:
                halves, have = spread(halves, (CORE, CORE), have)
                o, *halves = tie((o, *halves))
            h = (xs[c].astype(F32) + jnp.dot(o, wom, preferred_element_type=F32)).astype(BF16)
            u = _rms(h, ln2)
            u3 = u.reshape(tc, D // LANES, LANES)
            if c + 1 < NQ:
                u, u3, xs[c + 1] = tie((u, u3, xs[c + 1]))
            us.append(u)
            ug.append(lax.all_gather(u3, 'expert'))
            if c == 0:
                tok, gate, starts, counts = _routes(idx, g, E)
                ints = lax.all_gather(jnp.concatenate([starts, counts, jnp.pad(tok, (0, pad))]), 'expert')
                gate_all = lax.all_gather(jnp.pad(gate, (0, pad)), 'expert')[:, None, :]
                start = lax.dynamic_slice_in_dim(ints[:, :E], me * el, el, axis=1)
                cnt = lax.dynamic_slice_in_dim(ints[:, E:2 * E], me * el, el, axis=1)
                tok_all = ints[:, None, 2 * E:]
                start, cnt, tok_all, gate_all, xs[2] = tie((start, cnt, tok_all, gate_all, xs[2]))

        def devices(rel):
            return jnp.stack([me ^ rel, me ^ rel ^ CORE]).astype(jnp.int32)

        order = (X | Y, X, Y, 0)
        devs = {r: devices(r) for r in order}
        rows = _gather_rows(devs[order[0]], start, cnt, tok_all, ug, cap)
        S, got1, got2 = {}, {}, {}
        for i, r in enumerate(order):
            dev = devs[r]
            o = _experts(dev, cnt, rows, w1, w3, w2)
            other = _combine(dev[1:], 1, start, cnt, tok_all, gate_all, o, T, ())
            if i + 1 < len(order):
                nxt = order[i + 1]
                *other, devs[nxt] = tie((*other, devs[nxt]))
                rows = _gather_rows(devs[nxt], start, cnt, tok_all, ug, cap)
            other = [swap(p, CORE) for p in other]
            if i + 1 < len(order):
                *other, rows = tie((*other, rows))
            S[r] = _combine(dev[:1], 0, start, cnt, tok_all, gate_all, o, T, tuple(other))
            if i + 1 < len(order):
                *S[r], rows = tie((*S[r], rows))
            if r == (X | Y):
                got1[r] = (swap(S[r][0], X), swap(S[r][1], Y))
            elif r == X:
                got1[r] = swap(S[r][0], X)
                got2[r] = swap(S[r][1] + got1[X | Y][1], X)
            elif r == Y:
                got1[r] = swap(S[r][1], Y)
                got2[r] = swap(S[r][0] + got1[X | Y][0], Y)
                hb = jnp.concatenate(halves, axis=1)
                uu = jnp.concatenate(us, axis=0)
                ho = _ffn(uu[hot_tok], hb[0], hb[1], hb[2].reshape(FF, D)).astype(F32)
                hy = jnp.zeros((T, D), F32).at[hot_tok].set(hot_g[:, None] * ho)
                hy, rows = tie((hy, rows))

        return _final(hy, (S[0][0], got1[X], got2[Y]), (S[0][1], got1[Y], got2[X]))

    tk = ('data', 'expert')
    rep3 = P(None, None, None)
    exp3 = P('expert', None, None)
    return jax.shard_map(
        local, mesh=mesh,
        in_specs=(P(tk, None), P(tk, None), P(tk, None), P(tk), P(tk), P(None),
                  rep3, rep3, rep3, rep3, P(None), exp3, exp3, exp3),
        out_specs=P(tk, None), check_vma=False)
```
